32 devices in a mesh: row: 4 (over x, core), col: 8 (over z, y).
Axes of the slice: x: 2, y: 2, z: 4, core: 2. Of those that a mesh axis runs over, the one named last changes fastest.
Arguments:
- inputs: bfloat16 [512, 8192], P('col', 'row'), may hold values from -6 to 6
- cotangent: bfloat16 [512, 8192], P('col', 'row'), may hold values from -6 to 6
- gate_pre: bfloat16 [512, 16384], P('row', 'col'), may hold values from -8 to 8
- up_pre: bfloat16 [512, 16384], P('row', 'col'), may hold values from -6 to 6
- w_gate: bfloat16 [8192, 16384], P('row', 'col'), may hold values from -0.0625 to 0.0625
- w_up: bfloat16 [8192, 16384], P('row', 'col'), may hold values from -0.0625 to 0.0625
- w_down: bfloat16 [16384, 8192], P('col', 'row'), may hold values from -0.046875 to 0.046875
Outputs:
- grad_inputs: bfloat16 [512, 8192], P('col', 'row')
- grad_gate: float32 [8192, 16384], P('row', 'col')
- grad_up: float32 [8192, 16384], P('row', 'col')
- grad_down: float32 [16384, 8192], P('col', 'row')
The draws below stay inside these ranges and needn't reach their ends.
All inputs are finite; a program needn't handle non-finite values.
Results may differ from the reference program's by a relative error of at most 0.0049.
Values may be sent and summed in bfloat16 or wider, within the bound.
A program may use at most 128 MiB of HBM per device.

```python
import math
import jax
import jax.numpy as jnp

D = 8192
FF = 16384
TOKENS = 512


def block_scale(own_key, extent, shards, smallest, largest):
    gain = 1.0
    for axis_at, parts in shards:
        draws = jax.random.uniform(jax.random.fold_in(jax.random.fold_in(own_key, 6), axis_at), (parts,), jnp.float32, smallest / len(shards), largest / len(shards))
        gain = gain * jnp.repeat(jnp.exp(draws), extent[axis_at] // parts).reshape((-1,) + (1,) * (len(extent) - 1 - axis_at))
    return gain


def normal_values(own_key, dims, spread, most, cuts=(), kind=jnp.bfloat16):
    level = block_scale(own_key, dims, cuts, -0.22, 0.18) if cuts else 1.0
    entries = jax.random.normal(own_key, dims, jnp.float32) * spread * level
    return jnp.minimum(jnp.maximum(entries, -most), most).astype(kind)


def setup_inputs(seed: int = 0) -> dict:
    splits = jax.random.split(jax.random.key(seed), 8)
    return {
        "inputs": normal_values(splits[0], (TOKENS, D), 1.0, 6.0, ((0, 8), (1, 4))),
        "cotangent": normal_values(splits[1], (TOKENS, D), 1.0, 6.0, ((0, 8), (1, 4))),
        "gate_pre": normal_values(splits[2], (TOKENS, FF), 1.5, 8.0, ((0, 4), (1, 8))),
        "up_pre": normal_values(splits[3], (TOKENS, FF), 1.0, 6.0, ((0, 4), (1, 8))),
        "w_gate": normal_values(splits[4], (D, FF), D ** -0.5, 0.0625, ((0, 4), (1, 8))),
        "w_up": normal_values(splits[5], (D, FF), D ** -0.5, 0.0625, ((0, 4), (1, 8))),
        "w_down": normal_values(splits[6], (FF, D), FF ** -0.5, 0.046875, ((0, 8), (1, 4))),
    }


def reference(inputs, cotangent, gate_pre, up_pre, w_gate, w_up, w_down):
    gate_f = gate_pre.astype(jnp.float32)
    up_f = up_pre.astype(jnp.float32)
    sig = jax.nn.sigmoid(gate_f)
    act = gate_f * sig
    hidden = (act * up_f).astype(jnp.bfloat16)
    grad_hidden = jnp.dot(cotangent, w_down.T, preferred_element_type=jnp.float32)
    grad_gate_pre = (grad_hidden * up_f * sig * (1.0 + gate_f * (1.0 - sig))).astype(jnp.bfloat16)
    grad_up_pre = (grad_hidden * act).astype(jnp.bfloat16)
    grad_inputs = jnp.dot(grad_gate_pre, w_gate.T, preferred_element_type=jnp.float32)
    grad_inputs = grad_inputs + jnp.dot(grad_up_pre, w_up.T, preferred_element_type=jnp.float32)
    scale = 1.0 / math.sqrt(inputs.shape[0])
    grad_gate = jnp.dot(inputs.T, grad_gate_pre, preferred_element_type=jnp.float32) * scale
    grad_up = jnp.dot(inputs.T, grad_up_pre, preferred_element_type=jnp.float32) * scale
    grad_down = jnp.dot(hidden.T, cotangent, preferred_element_type=jnp.float32) * scale
    return (grad_inputs.astype(jnp.bfloat16), grad_gate, grad_up, grad_down)
```

```python
import math

import jax
import jax.numpy as jnp
from jax import lax
from jax.experimental import pallas as pl
from jax.experimental.pallas import tpu as pltpu
from jax.sharding import PartitionSpec as P


F32 = jnp.float32
BF16 = jnp.bfloat16
GRANT = 63 * 1024 * 1024
MESH = pl.DeviceIdType.MESH
ANY = pl.BlockSpec(memory_space=pl.ANY)
STEP = 16


def cuts_of(tc):
    return (tc // 2, tc // 2)


def dot_nt(left, right):
    return lax.dot_general(left, right, (((1,), (1,)), ((), ())), preferred_element_type=F32)


def tile_of(extent, most):
    tile = min(extent, most)
    while extent % tile:
        tile //= 2
    return tile


def pairs(sizes, inputs, cotangent, gate_pre, up_pre, w_gate, w_up, w_down):
    rows, cols = sizes
    groups, lines, q = rows // 2, cols // 2, cols // rows
    tc, F = inputs.shape
    _, H = gate_pre.shape
    T = tc * cols
    cuts = cuts_of(tc)
    starts = [sum(cuts[:i]) for i in range(len(cuts))]
    NCH = len(cuts)
    most = max(cuts) * cols

    def body(inp, cot, gate, up, wg, wu, wd,
             cot_o, x_o, hid_o, gg_o, gu_o, gi_o,
             cot_all, x_all, ga, ua, hid, gg, gu, wgv, wuv, wdv, lhs, lhs2,
             mine, theirs, recvd, xs, xr, ys, keep, yr, zs, zr, out, sem):
        r, c = lax.axis_index("row"), lax.axis_index("col")
        g, core, v, y = lax.div(r, 2), lax.rem(r, 2), lax.div(c, 2), lax.rem(c, 2)
        r_twin, c_twin = 2 * g + 1 - core, 2 * v + 1 - y
        count = [0]
        sent = []

        def new():
            count[0] += 1
            return sem.at[count[0] - 1]

        def local(src, dst):
            cp = pltpu.make_async_copy(src, dst, new())
            cp.start()
            return cp

        def remote(src, dst, to, recv):
            cp = pltpu.make_async_remote_copy(
                src_ref=src, dst_ref=dst, send_sem=new(), recv_sem=recv,
                device_id=to, device_id_type=MESH)
            cp.start()
            sent.append(cp)

        def arrive(dst, recv):
            pltpu.make_async_remote_copy(
                src_ref=dst, dst_ref=dst, send_sem=recv, recv_sem=recv,
                device_id=(r_twin, c), device_id_type=MESH).wait_recv()

        def v_at(k):
            return lax.rem(v + k + lines, lines)

        def g_at(k):
            return lax.rem(g + k + groups, groups)

        cot_in = [local(cot.at[s:s + n], cot_all.at[c, s:s + n]) for s, n in zip(starts, cuts)]
        gate_in = [
            [local(src.at[j * tc + s:j * tc + s + n], dst.at[g, j, s:s + n])
             for src, dst in ((gate, ga), (up, ua)) for j in range(q)]
            for s, n in zip(starts, cuts)]
        x_in = local(inp, x_all.at[c])
        wd_in = local(wd, wdv)
        wg_in = local(wg, wgv)
        wu_in = local(wu, wuv)

        barrier = pltpu.get_barrier_semaphore()
        peers = [(r_twin, c), (r, c_twin)]
        peers += [(2 * g_at(k) + core, c) for k in range(1, groups)]
        peers += [(r, 2 * v_at(k) + y) for k in range(1, lines)]
        for peer in peers:
            pl.semaphore_signal(barrier, inc=1, device_id=peer, device_id_type=MESH)
        pl.semaphore_wait(barrier, len(peers))

        cz_sem = [[new() for _ in range(lines)] for _ in cuts]
        cy_sem = [[new() for _ in range(lines)] for _ in cuts]
        xz_sem = [new() for _ in range(lines)]
        xy_sem = [new() for _ in range(lines)]
        gx_sem = [[[new() for _ in range(2 * q)] for _ in range(groups)] for _ in cuts]

        def send_gates(i):
            s, n = starts[i], cuts[i]
            for cp in gate_in[i]:
                cp.wait()
            for k in range(1, groups):
                for m, buf in enumerate((ga, ua)):
                    for j in range(q):
                        block = buf.at[g, j, s:s + n]
                        remote(block, block, (2 * g_at(k) + core, c), gx_sem[i][k][m * q + j])

        def send_cot(i):
            s, n = starts[i], cuts[i]
            cot_in[i].wait()
            block = cot_all.at[c, s:s + n]
            for k in range(1, lines):
                remote(block, block, (r, 2 * v_at(k) + y), cz_sem[i][k])
            remote(block, block, (r, c_twin), cy_sem[i][0])

        def forward_cot(i):
            s, n = starts[i], cuts[i]
            for k in range(1, lines):
                block = cot_all.at[2 * v_at(-k) + y, s:s + n]
                arrive(block, cz_sem[i][k])
                remote(block, block, (r, c_twin), cy_sem[i][k])

        def finish_cot(i):
            s, n = starts[i], cuts[i]
            for k in range(lines):
                arrive(cot_all.at[2 * v_at(-k) + 1 - y, s:s + n], cy_sem[i][k])

        def half_of(i):
            n = cuts[i]
            return groups * q * starts[i], groups * q * n

        tile_h, tile_f = tile_of(H, 512), tile_of(F, 512)
        d_sem = [new() for _ in cuts]

        def hidden_grad(i):
            s, n = starts[i], cuts[i]
            at, half = half_of(i)
            for h, side in enumerate((1 - core, core)):
                for m in range(groups):
                    first = (2 * m + side) * q
                    lhs[pl.ds(h * half + m * q * n, q * n), :F] = (
                        cot_all[pl.ds(first, q), s:s + n, :].reshape(q * n, F))

            def step(j, _):
                cut = pl.ds(pl.multiple_of(j * tile_h, tile_h), tile_h)
                got = dot_nt(lhs[:2 * half, :F], wdv[cut, :])
                theirs[at:at + half, cut] = got[:half]
                mine[at:at + half, cut] = got[half:]
                return 0

            lax.fori_loop(0, H // tile_h, step, 0)
            remote(theirs.at[at:at + half], recvd.at[at:at + half], (r_twin, c), d_sem[i])

        px_sem = [[new() for _ in range(groups)] for _ in cuts]

        def add_twin(i):
            at, half = half_of(i)
            arrive(recvd.at[at:at + half], d_sem[i])

            def step(j, _):
                cut = pl.ds(pl.multiple_of(at + j * STEP, STEP), STEP)
                total = mine[cut, :] + recvd[cut, :]
                mine[cut, :] = total
                xs[cut, :] = total.astype(BF16)
                return 0

            lax.fori_loop(0, half // STEP, step, 0)
            for k in range(1, groups):
                remote(xs.at[at:at + half], xr.at[k - 1, at:at + half],
                       (2 * g_at(k) + core, c), px_sem[i][k])

        u_sem = [[new() for _ in range(3 * groups)] for _ in cuts]

        def pointwise(i):
            s, n = starts[i], cuts[i]
            at, half = half_of(i)
            for k in range(1, groups):
                for m, buf in enumerate((ga, ua)):
                    for j in range(q):
                        arrive(buf.at[g_at(-k), j, s:s + n], gx_sem[i][k][m * q + j])
                arrive(xr.at[k - 1, at:at + half], px_sem[i][k])
            per = n // STEP

            def step(b, _):
                t, rest = lax.rem(b, per), lax.div(b, per)
                j, m = lax.rem(rest, q), lax.div(rest, q)
                here = pl.ds(pl.multiple_of(s + t * STEP, STEP), STEP)
                flat = pl.ds(pl.multiple_of(at + b * STEP, STEP), STEP)
                total = mine[flat, :]
                for k in range(1, groups):
                    total = total + xr[k - 1, flat, :].astype(F32)
                gate_f = ga[m, j, here, :].astype(F32)
                up_f = ua[m, j, here, :].astype(F32)
                sig = jax.nn.sigmoid(gate_f)
                act = gate_f * sig
                d = (2 * m + core) * q + j
                hid[d, here, :] = (act * up_f).astype(BF16)
                gu[d, here, :] = (total * act).astype(BF16)
                gg[d, here, :] = (total * (up_f * sig * (1.0 + gate_f * (1.0 - sig)))).astype(BF16)
                return 0

            lax.fori_loop(0, groups * q * per, step, 0)
            for e, buf in enumerate((gg, gu, hid)):
                for m in range(groups):
                    block = buf.at[pl.ds((2 * m + core) * q, q), s:s + n]
                    remote(block, block, (r_twin, c), u_sem[i][e * groups + m])

        def finish_twin(i, kinds):
            s, n = starts[i], cuts[i]
            for e in kinds:
                buf = (gg, gu, hid)[e]
                for m in range(groups):
                    arrive(buf.at[pl.ds((2 * m + 1 - core) * q, q), s:s + n], u_sem[i][e * groups + m])

        ry_sem = [new() for _ in cuts]

        def input_grad(i):
            s, n = starts[i], cuts[i]
            half = lines * n
            at = lines * s
            for h, side in enumerate((1 - y, y)):
                for k in range(lines):
                    d = 2 * v_at(k) + side
                    lhs[pl.ds(h * half + k * n, n), :H] = gg[d, s:s + n, :]
                    lhs2[pl.ds(h * half + k * n, n), :] = gu[d, s:s + n, :]

            def step(j, _):
                cut = pl.ds(pl.multiple_of(j * tile_f, tile_f), tile_f)
                got = dot_nt(lhs[:2 * half, :H], wgv[cut, :]) + dot_nt(lhs2[:2 * half, :], wuv[cut, :])
                ys[at:at + half, cut] = got[:half].astype(BF16)
                keep[at:at + half, cut] = got[half:]
                return 0

            lax.fori_loop(0, F // tile_f, step, 0)
            remote(ys.at[at:at + half], yr.at[at:at + half], (r, c_twin), ry_sem[i])

        rz_sem = [[new() for _ in range(lines)] for _ in cuts]

        def add_line(i):
            s, n = starts[i], cuts[i]
            at = lines * s
            arrive(yr.at[at:at + lines * n], ry_sem[i])
            for k in list(range(1, lines)) + [0]:
                def step(j, _):
                    flat = pl.ds(pl.multiple_of(at + k * n + j * STEP, STEP), STEP)
                    total = keep[flat, :] + yr[flat, :].astype(F32)
                    if k:
                        zs[k - 1, pl.ds(pl.multiple_of(s + j * STEP, STEP), STEP), :] = total.astype(BF16)
                    else:
                        keep[flat, :] = total
                    return 0

                lax.fori_loop(0, n // STEP, step, 0)
                if k:
                    remote(zs.at[k - 1, s:s + n], zr.at[k - 1, s:s + n],
                           (r, 2 * v_at(k) + y), rz_sem[i][k])

        def finish_line(i):
            s, n = starts[i], cuts[i]
            at = lines * s
            for k in range(1, lines):
                arrive(zr.at[k - 1, s:s + n], rz_sem[i][k])

            def step(j, _):
                here = pl.ds(pl.multiple_of(s + j * STEP, STEP), STEP)
                total = keep[pl.ds(pl.multiple_of(at + j * STEP, STEP), STEP), :]
                for k in range(1, lines):
                    total = total + zr[k - 1, here, :].astype(F32)
                out[here, :] = total.astype(BF16)
                return 0

            lax.fori_loop(0, n // STEP, step, 0)
            outs.append(local(out.at[s:s + n], gi_o.at[s:s + n]))

        def send_x_lines():
            x_in.wait()
            block = x_all.at[c]
            for k in range(1, lines):
                remote(block, block, (r, 2 * v_at(k) + y), xz_sem[k])

        def send_x_twin():
            block = x_all.at[c]
            remote(block, block, (r, c_twin), xy_sem[0])

        def forward_x():
            for k in range(1, lines):
                block = x_all.at[2 * v_at(-k) + y]
                arrive(block, xz_sem[k])
                remote(block, block, (r, c_twin), xy_sem[k])

        def finish_x():
            for k in range(lines):
                arrive(x_all.at[2 * v_at(-k) + 1 - y], xy_sem[k])

        outs = []
        for i in range(NCH):
            send_cot(i)
            if i < 2:
                send_gates(i)
        send_x_lines()
        forward_cot(0)
        finish_cot(0)
        wd_in.wait()
        for i in range(NCH):
            hidden_grad(i)
            if i + 1 < NCH:
                forward_cot(i + 1)
            add_twin(i)
            if i + 2 < NCH:
                send_gates(i + 2)
            if i + 1 < NCH:
                finish_cot(i + 1)
        send_x_twin()
        outs.append(local(cot_all, cot_o))
        wg_in.wait()
        wu_in.wait()
        for i in range(NCH):
            pointwise(i)
            if i == 0:
                forward_x()
            finish_twin(i, (0, 1))
            input_grad(i)
            if i:
                add_line(i - 1)
        finish_twin(0, (2,))
        for i in range(1, NCH):
            finish_twin(i, (2,))
        outs += [local(hid, hid_o), local(gg, gg_o), local(gu, gu_o)]
        finish_x()
        outs.append(local(x_all, x_o))
        add_line(NCH - 1)
        for i in range(NCH):
            finish_line(i)
        for cp in sent:
            cp.wait_send()
        for cp in outs:
            cp.wait()

    halfT = T // 2
    scratch = [
        pltpu.VMEM((cols, tc, F), BF16), pltpu.VMEM((cols, tc, F), BF16),
        pltpu.VMEM((groups, q, tc, H), BF16), pltpu.VMEM((groups, q, tc, H), BF16),
        pltpu.VMEM((cols, tc, H), BF16), pltpu.VMEM((cols, tc, H), BF16), pltpu.VMEM((cols, tc, H), BF16),
        pltpu.VMEM((F, H), BF16), pltpu.VMEM((F, H), BF16), pltpu.VMEM((H, F), BF16),
        pltpu.VMEM((most, max(F, H)), BF16), pltpu.VMEM((most, H), BF16),
        pltpu.VMEM((halfT, H), F32), pltpu.VMEM((halfT, H), F32), pltpu.VMEM((halfT, H), F32),
        pltpu.VMEM((halfT, H), BF16), pltpu.VMEM((groups - 1, halfT, H), BF16),
        pltpu.VMEM((halfT, F), BF16), pltpu.VMEM((halfT, F), F32), pltpu.VMEM((halfT, F), BF16),
        pltpu.VMEM((lines - 1, tc, F), BF16), pltpu.VMEM((lines - 1, tc, F), BF16),
        pltpu.VMEM((tc, F), BF16),
    ]
    sems = 12 + NCH * (1 + 2 * q + 4 * lines + 4 * (groups - 1) * q + 2 * groups * q + 2 * groups + 2 + 6 * groups
                       + 2 + 2 * lines) + 4 * lines + 8
    scratch.append(pltpu.SemaphoreType.DMA((sems,)))
    wide = [jax.ShapeDtypeStruct((cols, tc, n), BF16) for n in (F, F, H, H, H)]
    args = (inputs, cotangent, gate_pre, up_pre, w_gate, w_up, w_down)
    got = pl.pallas_call(
        body,
        in_specs=[ANY] * 7,
        out_specs=[ANY] * 6,
        out_shape=wide + [jax.ShapeDtypeStruct((tc, F), BF16)],
        scratch_shapes=scratch,
        compiler_params=pltpu.CompilerParams(
            collective_id=0, has_side_effects=True, vmem_limit_bytes=GRANT),
        cost_estimate=pl.CostEstimate(flops=6 * T * F * H, bytes_accessed=60 << 20, transcendentals=0),
        name="pairs",
    )(*args)
    return [a.reshape(T, -1) for a in got[:5]] + [got[5]]


def outer(left, right, scale):
    tokens, wide = right.shape
    spread = left.shape[-1]
    tile = tile_of(spread, 512)

    def body(left_ref, right_ref, out):
        out[...] = lax.dot_general(
            left_ref[...], right_ref[...], (((0,), (0,)), ((), ())), preferred_element_type=F32
        ) * scale

    return pl.pallas_call(
        body,
        grid=(spread // tile,),
        in_specs=[pl.BlockSpec((tokens, tile), lambda i: (0, i)),
                  pl.BlockSpec((tokens, wide), lambda i: (0, 0))],
        out_specs=pl.BlockSpec((tile, wide), lambda i: (i, 0)),
        out_shape=jax.ShapeDtypeStruct((spread, wide), F32),
        compiler_params=pltpu.CompilerParams(
            dimension_semantics=("arbitrary",), vmem_limit_bytes=GRANT),
        cost_estimate=pl.CostEstimate(
            flops=2 * tokens * spread * wide, bytes_accessed=4 * spread * wide, transcendentals=0),
    )(left, right)


def solution(mesh):
    sizes = (mesh.shape["row"], mesh.shape["col"])
    in_specs = (
        P("col", "row"),
        P("col", "row"),
        P("row", "col"),
        P("row", "col"),
        P("row", "col"),
        P("row", "col"),
        P("col", "row"),
    )
    out_specs = (P("col", "row"), P("row", "col"), P("row", "col"), P("col", "row"))

    def body(*args):
        cot_all, x_all, hid, gg, gu, grad_inputs = pairs(sizes, *args)
        scale = 1.0 / math.sqrt(cot_all.shape[0])
        grad_down = outer(hid, cot_all, scale)
        grad_gate = outer(x_all, gg, scale)
        grad_up = outer(x_all, gu, scale)
        return grad_inputs, grad_gate, grad_up, grad_down

    return jax.shard_map(body, mesh=mesh, in_specs=in_specs, out_specs=out_specs, check_vma=False)
```
